32 devices in a mesh: rep: 2 (over x), section: 2 (over core), wide: 8 (over z, y).
Axes of the slice: x: 2, y: 2, z: 4, core: 2. Of those that a mesh axis runs over, the one named last changes fastest.
Arguments:
- acts: bfloat16 [2, 128, 8192], P('section', 'rep', 'wide'), parts along dimension 1, may hold values from -100 to 100
- norm_gain: bfloat16 [2, 8192], P('section', 'wide'), may hold values from 0.099609375 to 1.8984375
- w_qkv: bfloat16 [2, 8192, 5120], P('section', None, 'wide'), may hold values from -0.0625 to 0.0625
- w_out: bfloat16 [2, 4096, 8192], P('section', None, 'wide'), may hold values from -0.5 to 0.5
- key_cache: bfloat16 [2, 128, 384, 512], P('section', ('rep', 'wide')), parts along dimension 1, may hold values from -400 to 400
- value_cache: bfloat16 [2, 128, 384, 512], P('section', ('rep', 'wide')), parts along dimension 1, may hold values from -6 to 6
- cache_lengths: int32 [2, 128], P('section', ('rep', 'wide')), parts along dimension 1, may hold values from 2 to 384, as said below
- slot_of: int32 [2, 128], P('section', 'rep'), parts along dimension 1, may hold values from 0 to 63, each once within a row
Outputs:
- handed: bfloat16 [2, 128, 8192], P('section', 'rep', 'wide'), parts along dimension 1
The draws below stay inside these ranges and needn't reach their ends.
There are 2 independent parts, one for each index of `rep`. The reference program is written for one: setup_inputs(seed, part) draws one part's arguments, and reference() takes and returns one part's arrays. A program takes and returns all parts, laid end to end along the dimension named above; an argument that names none is the same for every part. Nothing has to cross between parts.
Inputs may be any that keep to these rules, and one draw needn't show every extreme that they name: `cache_lengths`: slot j of a section belongs to owner j // 8; in every section some slot holds exactly 384. `slot_of`: each section's row names every slot once.
All inputs are finite; a program needn't handle non-finite values.
Results may differ from the reference program's by a relative error of at most 0.005.
Values may be sent and summed in bfloat16 or wider, within the bound.
A program may use at most 64 MiB of HBM per device.

```python
import math
import jax
import jax.numpy as jnp
from jax import lax

D = 8192
HEADS = 32
KV_HEADS = 4
HDIM = 128
LMAX = 384
REQ_DEV = 8
SECTIONS = 2
REQUESTS = 64
QKV = 5120


def draw_acts(key, part):
    streams = jax.random.split(key, 4)
    values_raw = jax.random.normal(streams[0], (SECTIONS, REQUESTS, D), jnp.float32)
    column = jnp.arange(D, dtype=jnp.float32) / max(D - 1, 1)
    jitter = jnp.exp(jax.random.uniform(streams[3], (SECTIONS, 1, D), jnp.float32, -0.6, 0.6))
    column_rise = jnp.exp(math.log(3.0) * column)
    row_scale = jnp.exp(jax.random.uniform(streams[1], (SECTIONS, REQUESTS, 1), jnp.float32, math.log(0.3), math.log(3.0)))
    return jnp.clip(values_raw * row_scale * column_rise * jitter, -100.0, 100.0).astype(jnp.bfloat16)


def draw_key_cache(key, part):
    streams = jax.random.split(key, 1)
    width_all = KV_HEADS * HDIM
    values_raw = jnp.clip(jax.random.normal(streams[0], (SECTIONS, REQUESTS, LMAX, width_all), jnp.float32), -6.0, 6.0)
    return jnp.clip(values_raw, -400.0, 400.0).astype(jnp.bfloat16)


def draw_cache_lengths(key, part):
    streams = jax.random.split(key, 3)
    owners = REQUESTS // REQ_DEV
    shifts = jax.random.randint(streams[0], (SECTIONS, owners, 1), 0, 4)
    ceiling = jnp.maximum(jnp.right_shift(jnp.int32(LMAX), shifts), 2)
    lengths_raw = 2 + jax.random.randint(streams[1], (SECTIONS, owners, REQ_DEV), 0, ceiling - 1)
    lengths_flat = lengths_raw.reshape(SECTIONS, REQUESTS)
    chosen = jax.random.randint(streams[2], (SECTIONS,), 0, REQUESTS)
    section_rows = jnp.arange(SECTIONS, dtype=jnp.int32)
    lengths_flat = lengths_flat.at[section_rows, chosen].set(LMAX)
    return lengths_flat.astype(jnp.int32)


def shard_levels(own_key, extent, pieces, smallest, top_value):
    loudness, own = 1.0, jax.random.fold_in(own_key, 6)
    for axis_at, blocks in pieces:
        draws = jnp.exp(jax.random.uniform(jax.random.fold_in(own, axis_at), (blocks,), jnp.float32, smallest / len(pieces), top_value / len(pieces)))
        loudness = loudness * jnp.repeat(draws, extent[axis_at] // blocks).reshape([-1 if axis == axis_at else 1 for axis in range(len(extent))])
    return loudness


def centred(own_key, dims, scale, reach, pieces=(), kind=jnp.bfloat16):
    result = scale * jax.random.normal(own_key, dims, jnp.float32)
    if pieces:
        result = result * shard_levels(own_key, dims, pieces, -0.22, 0.18)
    return jnp.clip(result, -reach, reach).astype(kind)


def setup_inputs(seed: int = 0, part: int = 0) -> dict:
    arg_keys = jax.random.split(jax.random.key(seed), 9)
    own_keys = jax.random.split(jax.random.fold_in(arg_keys[8], part), 9)
    acts = draw_acts(jax.random.fold_in(jax.random.fold_in(arg_keys[8], part), 71), part)
    norm_gain = jnp.clip(1.0 + 0.18 * jax.random.normal(arg_keys[1], (SECTIONS, D), jnp.float32), 0.099609375, 1.8984375).astype(jnp.bfloat16)
    w_qkv = centred(arg_keys[2], (SECTIONS, D, QKV), D ** -0.5, 0.0625, ((0, 2), (2, 8)))
    w_out = centred(arg_keys[3], (SECTIONS, HEADS * HDIM, D), HDIM ** -0.5, 0.5, ((0, 2), (2, 8)))
    key_cache = draw_key_cache(jax.random.fold_in(jax.random.fold_in(arg_keys[8], part), 71), part)
    value_cache = centred(own_keys[5], (SECTIONS, REQUESTS, LMAX, KV_HEADS * HDIM), 1.0, 6.0, ((0, 2), (1, 8)))
    cache_lengths = draw_cache_lengths(jax.random.fold_in(jax.random.fold_in(arg_keys[8], part), 71), part)
    slot_of = jax.vmap(lambda own: jax.random.permutation(own, REQUESTS))(jax.random.split(own_keys[7], SECTIONS)).reshape((SECTIONS, REQUESTS)).astype(jnp.int32)
    return {"acts": acts, "norm_gain": norm_gain, "w_qkv": w_qkv, "w_out": w_out, "key_cache": key_cache, "value_cache": value_cache, "cache_lengths": cache_lengths, "slot_of": slot_of}


epsilon = 1e-05
rope_base = 500000.0
masked_score = -1e+30

def rounded(values):
    return lax.optimization_barrier(values.astype(jnp.bfloat16)).astype(jnp.float32)

def rotate(values, position):
    half_dim = HDIM // 2
    exponent = jnp.arange(half_dim, dtype=jnp.float32) * (2.0 / HDIM)
    frequency = jnp.exp(-math.log(rope_base) * exponent)
    angle = position[..., None] * frequency
    cosine = jnp.cos(angle)
    sine = jnp.sin(angle)
    first_half = values[..., :half_dim]
    second_half = values[..., half_dim:]
    return jnp.concatenate([first_half * cosine - second_half * sine, second_half * cosine + first_half * sine], axis=-1)

def attend(joined_rows, key_rows, value_rows, lengths_here):
    row_count = joined_rows.shape[0]
    groups = HEADS // KV_HEADS
    query_width = HEADS * HDIM
    kv_width = KV_HEADS * HDIM
    queries = joined_rows[:, :query_width].reshape(row_count, KV_HEADS, groups, HDIM).astype(jnp.float32)
    new_keys = joined_rows[:, query_width:query_width + kv_width].reshape(row_count, KV_HEADS, HDIM).astype(jnp.float32)
    new_values = joined_rows[:, query_width + kv_width:].reshape(row_count, KV_HEADS, HDIM).astype(jnp.float32)
    position = lengths_here.astype(jnp.float32)
    query_wide = rounded(rotate(queries, position[:, None, None]))
    key_wide = rounded(rotate(new_keys, position[:, None]))
    score_scale = 1.0 / math.sqrt(HDIM)
    cache_span = key_rows.shape[1]
    cached_keys = key_rows.reshape(row_count, cache_span, KV_HEADS, HDIM).astype(jnp.float32)
    cached_values = value_rows.reshape(row_count, cache_span, KV_HEADS, HDIM).astype(jnp.float32)
    scores = jnp.einsum('ngqd,nlgd->ngql', query_wide, cached_keys) * score_scale
    own_score = jnp.einsum('ngqd,ngd->ngq', query_wide, key_wide) * score_scale
    live_mask = (jnp.arange(cache_span, dtype=jnp.int32)[None, :] < lengths_here[:, None])[:, None, None, :]
    masked = jnp.where(live_mask, scores, masked_score)
    peak = jnp.maximum(lax.optimization_barrier(jnp.max(masked, axis=-1)), own_score)
    weights = jnp.where(live_mask, jnp.exp(masked - peak[..., None]), 0.0)
    own_weight = jnp.exp(own_score - peak)
    denominator = lax.optimization_barrier(jnp.sum(weights, axis=-1)) + own_weight
    weighted = jnp.einsum('ngql,nlgd->ngqd', rounded(weights), cached_values)
    weighted = weighted + rounded(own_weight)[..., None] * new_values[:, :, None, :]
    return (weighted / denominator[..., None]).reshape(row_count, query_width).astype(jnp.bfloat16)

def reference(acts, norm_gain, w_qkv, w_out, key_cache, value_cache, cache_lengths, slot_of):
    results = []
    for section_index in range(SECTIONS):
        tokens = acts[section_index].astype(jnp.float32)
        squares = lax.optimization_barrier(jnp.sum(tokens * tokens, axis=1))
        normed = (tokens * lax.rsqrt(squares / D + epsilon)[:, None] * norm_gain[section_index].astype(jnp.float32)).astype(jnp.bfloat16)
        joined_rows = jnp.dot(normed, w_qkv[section_index], preferred_element_type=jnp.float32).astype(jnp.bfloat16)
        slot_table = slot_of[section_index]
        request_at_slot = jnp.zeros((REQUESTS,), jnp.int32).at[slot_table].set(jnp.arange(REQUESTS, dtype=jnp.int32))
        attended = attend(joined_rows[request_at_slot], key_cache[section_index], value_cache[section_index], cache_lengths[section_index])
        projected = jnp.dot(attended[slot_table], w_out[section_index], preferred_element_type=jnp.float32)
        results.append((tokens + projected).astype(jnp.bfloat16))
    return jnp.stack([results[-1]] + results[:-1])
```

```python
import functools
import math

import jax
import jax.numpy as jnp
from jax import lax
from jax.experimental import pallas as pl
from jax.experimental.pallas import tpu as pltpu
from jax.sharding import PartitionSpec as P

D = 8192
HEADS = 32
KV_HEADS = 4
HDIM = 128

epsilon = 1e-05
rope_base = 500000.0
masked_score = -1e30

MESH = pl.DeviceIdType.MESH


def tick(
    n, Y, C, sections,
    acts_ref, gain_ref, slot_ref, len_ref, wq_hbm, wo_hbm, k_hbm, v_hbm, out_hbm,
    wq, wo, kc, vc, xa, acc, js, jr, sqs, sqr, qs, at, ga, res,
    wq_sem, wo_sem, k_sem, v_sem,
    x_sz, x_sy, x_rv, j_sn, j_rv, q_sn, q_rv, a_sz, a_sy, a_rv, o_sn, o_rv,
):
    me = lax.axis_index("wide")
    sec = lax.axis_index("section")
    Z = n // Y
    z, y = me // Y, lax.rem(me, Y)
    other = z * Y + (1 - y)
    rows, width = acts_ref.shape[1], acts_ref.shape[2]
    CK = width // C
    G = KV_HEADS
    heads = HEADS // G
    own = rows // n
    cols = wq.shape[1]
    slabs = cols // HDIM
    out_chunks = res.shape[0]
    OC = res.shape[2]

    barrier = pltpu.get_barrier_semaphore()
    for step in range(1, n):
        pl.semaphore_signal(
            barrier, inc=1, device_id={"wide": lax.rem(me + step, n)}, device_id_type=MESH
        )
    pl.semaphore_signal(
        barrier, inc=1, device_id={"section": lax.rem(sec + 1, sections)}, device_id_type=MESH
    )

    def wq_copy(b):
        at_rows = pl.ds(pl.multiple_of(b * width, width), width)
        return pltpu.make_async_copy(wq_hbm.at[0, at_rows, :], wq.at[at_rows, :], wq_sem.at[b])

    for step in range(n):
        wq_copy(lax.rem(me + step, n)).start()
    k_copy = pltpu.make_async_copy(k_hbm.at[0], kc, k_sem)
    v_copy = pltpu.make_async_copy(v_hbm.at[0], vc, v_sem)
    wo_copy = pltpu.make_async_copy(wo_hbm.at[0], wo, wo_sem)
    k_copy.start()
    v_copy.start()
    wo_copy.start()

    tokens = acts_ref[0].astype(jnp.float32)
    gained = (tokens * gain_ref[...].astype(jnp.float32)).astype(jnp.bfloat16)
    for c in range(C):
        xa[me, c] = gained[:, c * CK : (c + 1) * CK]
    squares = jnp.sum(tokens * tokens, axis=1, keepdims=True)
    sub = lax.broadcasted_iota(jnp.int32, (rows, rows), 0)
    lane = lax.broadcasted_iota(jnp.int32, (rows, rows), 1)
    square_row = jnp.sum(jnp.where(sub == lane, squares, 0.0), axis=0, keepdims=True)
    to_slot_mask = sub == slot_ref[...]
    square_slot = jnp.sum(jnp.where(to_slot_mask, square_row, 0.0), axis=1, keepdims=True)
    square_wide = jnp.broadcast_to(square_slot, (rows, HDIM))
    for o in range(n):
        sqs[o] = square_wide[o * own : (o + 1) * own]
    to_slot_f = jnp.where(to_slot_mask, 1.0, 0.0)
    to_slot = to_slot_f.astype(jnp.bfloat16)
    to_request = to_slot_f.T.astype(jnp.bfloat16)

    pl.semaphore_wait(barrier, n)

    def remote(src, dst, send, recv, target):
        return pltpu.make_async_remote_copy(
            src_ref=src, dst_ref=dst, send_sem=send, recv_sem=recv,
            device_id={"wide": target}, device_id_type=MESH,
        )

    def x_z(dz, c):
        return remote(
            xa.at[me, c], xa.at[me, c], x_sz.at[dz, c], x_rv.at[me, c],
            lax.rem(z + dz, Z) * Y + y,
        )

    def x_y(zb, c):
        b = zb * Y + y
        return remote(xa.at[b, c], xa.at[b, c], x_sy.at[zb, c], x_rv.at[b, c], other)

    def x_wait(b, c):
        remote(xa.at[b, c], xa.at[b, c], x_sy.at[0, c], x_rv.at[b, c], other).wait_recv()

    for c in range(C):
        x_y(z, c).start()
        for dz in range(1, Z):
            x_z(dz, c).start()

    def q_copy(step):
        o = lax.rem(me + step, n)
        return remote(sqs.at[o], sqr.at[me], q_sn.at[step], q_rv.at[me], o)

    for step in range(1, n):
        q_copy(step).start()
    sqr[me] = sqs[me]

    def piece(b, c):
        at_rows = pl.ds(pl.multiple_of(b * width + c * CK, CK), CK)
        return jnp.dot(xa[b, c], wq[at_rows, :], preferred_element_type=jnp.float32)

    for step in range(n):
        wq_copy(lax.rem(me + step, n)).wait()

    total = piece(me, 0)
    for c in range(1, C):
        total += piece(me, c)
    acc[...] = total

    def other_line(c):
        for dz in range(Z):
            x_wait(lax.rem(z + dz, Z) * Y + (1 - y), c)
        part = acc[...]
        for dz in range(Z):
            part += piece(lax.rem(z + dz, Z) * Y + (1 - y), c)
        acc[...] = part

    def gather_step(c, carry):
        for dz in range(1, Z):
            zb = lax.rem(z + dz, Z)
            x_wait(zb * Y + y, c)
            x_y(zb, c).start()
        part = acc[...]
        for dz in range(1, Z):
            part += piece(lax.rem(z + dz, Z) * Y + y, c)
        acc[...] = part

        @pl.when(c > 0)
        def _():
            other_line(c - 1)

        return carry

    lax.fori_loop(0, C, gather_step, 0)
    other_line(C - 1)

    by_slot = jnp.dot(to_slot, acc[...].astype(jnp.bfloat16), preferred_element_type=jnp.float32)
    for o in range(n):
        js[o] = by_slot[o * own : (o + 1) * own].astype(jnp.bfloat16)

    def j_copy(step):
        o = lax.rem(me + step, n)
        return remote(js.at[o], jr.at[me], j_sn.at[step], j_rv.at[me], o)

    for step in range(1, n):
        j_copy(step).start()
    jr[me] = js[me]

    row_of = lax.broadcasted_iota(jnp.int32, (own, HDIM), 0)
    lane_of = lax.broadcasted_iota(jnp.int32, (own, HDIM), 1)
    position = jnp.zeros((own, HDIM), jnp.int32)
    for r in range(own):
        position = jnp.where(row_of == r, len_ref[0, r], position)
    half = lax.rem(lane_of, HDIM // 2).astype(jnp.float32) * (2.0 / HDIM)
    angle = position.astype(jnp.float32) * jnp.exp(-math.log(rope_base) * half)
    cosine = jnp.cos(angle)
    sine = jnp.where(lane_of < HDIM // 2, -jnp.sin(angle), jnp.sin(angle))
    k_copy.wait()
    v_copy.wait()
    wo_copy.wait()

    for step in range(1, n):
        b = lax.rem(me + step, n)
        remote(sqs.at[b], sqr.at[b], q_sn.at[step], q_rv.at[b], b).wait_recv()
    square_sum = sqr[0]
    for b in range(1, n):
        square_sum += sqr[b]
    scale = lax.rsqrt(square_sum / D + epsilon)
    for step in range(1, n):
        b = lax.rem(me + step, n)
        remote(js.at[b], jr.at[b], j_sn.at[step], j_rv.at[b], b).wait_recv()
    for b in range(n):
        for k in range(slabs):
            feature = b * slabs + k
            slab = jr[b, :, k * HDIM : (k + 1) * HDIM].astype(jnp.float32) * scale
            if feature < HEADS + G:
                turned = slab * cosine + pltpu.roll(slab, HDIM // 2, 1) * sine
                slab = turned.astype(jnp.bfloat16).astype(jnp.float32)
            else:
                slab = slab.astype(jnp.bfloat16).astype(jnp.float32)
            qs[:, feature, :] = slab

    def a_z(g, dz):
        return remote(
            ga.at[g, me], ga.at[g, me], a_sz.at[g, dz], a_rv.at[g, me],
            lax.rem(z + dz, Z) * Y + y,
        )

    def a_y(g, zb):
        b = zb * Y + y
        return remote(ga.at[g, b], ga.at[g, b], a_sy.at[g, zb], a_rv.at[g, b], other)

    def a_wait(g, b):
        remote(ga.at[g, b], ga.at[g, b], a_sy.at[g, 0], a_rv.at[g, b], other).wait_recv()

    def relay(g):
        for dz in range(1, Z):
            zb = lax.rem(z + dz, Z)
            a_wait(g, zb * Y + y)
            a_y(g, zb).start()

    span = kc.shape[1]
    score_scale = 1.0 / math.sqrt(HDIM)
    place = lax.broadcasted_iota(jnp.int32, (heads, span), 1)
    for g in range(G):
        lanes = slice(g * HDIM, (g + 1) * HDIM)
        for r in range(own):
            query = qs[r, g * heads : (g + 1) * heads, :]
            new_key = qs[r, HEADS + g : HEADS + g + 1, :]
            new_value = qs[r, HEADS + G + g : HEADS + G + g + 1, :]
            own_score = jnp.sum(query * new_key, axis=1, keepdims=True) * score_scale
            scores = (
                lax.dot_general(
                    query.astype(jnp.bfloat16), kc[r, :, lanes], (((1,), (1,)), ((), ())),
                    preferred_element_type=jnp.float32,
                )
                * score_scale
            )
            live = place < len_ref[0, r]
            masked = jnp.where(live, scores, masked_score)
            peak = jnp.maximum(jnp.max(masked, axis=1, keepdims=True), own_score)
            weights = jnp.where(live, jnp.exp(masked - peak), 0.0)
            own_weight = jnp.exp(own_score - peak)
            denominator = jnp.sum(weights, axis=1, keepdims=True) + own_weight
            weighted = jnp.dot(
                weights.astype(jnp.bfloat16), vc[r, :, lanes], preferred_element_type=jnp.float32
            )
            weighted += own_weight.astype(jnp.bfloat16).astype(jnp.float32) * new_value
            at[g, r] = weighted / denominator
        for h in range(heads):
            ga[g, me, :, h * HDIM : (h + 1) * HDIM] = at[g, :, h, :].astype(jnp.bfloat16)
        a_y(g, z).start()
        for dz in range(1, Z):
            a_z(g, dz).start()
        if g >= 2:
            relay(g - 2)
    for g in range(max(G - 2, 0), G):
        relay(g)

    def o_copy(c):
        return pltpu.make_async_remote_copy(
            src_ref=res.at[c],
            dst_ref=out_hbm.at[0, :, pl.ds(c * OC, OC)],
            send_sem=o_sn.at[c],
            recv_sem=o_rv.at[c],
            device_id={"section": lax.rem(sec + 1, sections)},
            device_id_type=MESH,
        )

    depth = heads * HDIM
    mixed = []
    for g in range(G):
        for dz in range(Z):
            a_wait(g, lax.rem(z + dz, Z) * Y + (1 - y))
        block = ga[g].astype(jnp.float32).reshape(rows, depth).astype(jnp.bfloat16)
        mixed.append(
            jnp.dot(to_request, block, preferred_element_type=jnp.float32).astype(jnp.bfloat16)
        )
        if g == G - 1:
            whole = jnp.concatenate(mixed, axis=1)
            for c in range(out_chunks):
                at_cols = slice(c * OC, (c + 1) * OC)
                part = acts_ref[0, :, at_cols].astype(jnp.float32)
                part += jnp.dot(whole, wo[:, at_cols], preferred_element_type=jnp.float32)
                res[c] = part.astype(jnp.bfloat16)
                o_copy(c).start()

    for c in range(C):
        for dz in range(1, Z):
            x_z(dz, c).wait_send()
        for zb in range(Z):
            x_y(zb, c).wait_send()
    for step in range(1, n):
        q_copy(step).wait_send()
        j_copy(step).wait_send()
    for g in range(G):
        for dz in range(1, Z):
            a_z(g, dz).wait_send()
        for zb in range(Z):
            a_y(g, zb).wait_send()
    for c in range(out_chunks):
        o_copy(c).wait()


def fused(n, sections, acts, norm_gain, w_qkv, w_out, key_cache, value_cache, cache_lengths, slot_of):
    Y, C, out_chunks = 2, 4, 4
    rows, width = acts.shape[1:]
    own, span, kv_width = key_cache.shape[1:]
    cols = w_qkv.shape[2]
    G = KV_HEADS
    heads = HEADS // G
    Z = n // Y
    vmem = pl.BlockSpec(memory_space=pltpu.VMEM)
    smem = pl.BlockSpec(memory_space=pltpu.SMEM)
    anywhere = pl.BlockSpec(memory_space=pl.ANY)
    bf16, f32 = jnp.bfloat16, jnp.float32
    dma = pltpu.SemaphoreType.DMA
    return pl.pallas_call(
        functools.partial(tick, n, Y, C, sections),
        out_shape=jax.ShapeDtypeStruct(acts.shape, bf16),
        in_specs=[vmem, vmem, vmem, smem, anywhere, anywhere, anywhere, anywhere],
        out_specs=anywhere,
        scratch_shapes=[
            pltpu.VMEM(w_qkv.shape[1:], bf16),
            pltpu.VMEM(w_out.shape[1:], bf16),
            pltpu.VMEM(key_cache.shape[1:], bf16),
            pltpu.VMEM(value_cache.shape[1:], bf16),
            pltpu.VMEM((n, C, rows, width // C), bf16),
            pltpu.VMEM((rows, cols), f32),
            pltpu.VMEM((n, own, cols), bf16),
            pltpu.VMEM((n, own, cols), bf16),
            pltpu.VMEM((n, own, HDIM), f32),
            pltpu.VMEM((n, own, HDIM), f32),
            pltpu.VMEM((own, HEADS + 2 * G, HDIM), f32),
            pltpu.VMEM((G, own, heads, HDIM), f32),
            pltpu.VMEM((G, n, own, heads * HDIM), bf16),
            pltpu.VMEM((out_chunks, rows, width // out_chunks), bf16),
            dma((n,)), dma, dma, dma,
            dma((Z, C)), dma((Z, C)), dma((n, C)),
            dma((n,)), dma((n,)), dma((n,)), dma((n,)),
            dma((G, Z)), dma((G, Z)), dma((G, n)),
            dma((out_chunks,)), dma((out_chunks,)),
        ],
        compiler_params=pltpu.CompilerParams(
            collective_id=0, has_side_effects=True, vmem_limit_bytes=60 * 1024 * 1024
        ),
    )(acts, norm_gain, slot_of, cache_lengths, w_qkv, w_out, key_cache, value_cache)


def passed_along(value, axis, steps):
    count = lax.axis_size(axis)
    pairs = [(source, (source + steps) % count) for source in range(count)]
    return lax.ppermute(value, axis, pairs)


def rotate(values, position):
    half_dim = HDIM // 2
    exponent = jnp.arange(half_dim, dtype=jnp.float32) * (2.0 / HDIM)
    frequency = jnp.exp(-math.log(rope_base) * exponent)
    angle = position[..., None] * frequency
    cosine = jnp.cos(angle)
    sine = jnp.sin(angle)
    first_half = values[..., :half_dim]
    second_half = values[..., half_dim:]
    return jnp.concatenate(
        [first_half * cosine - second_half * sine, second_half * cosine + first_half * sine],
        axis=-1,
    )


def attend(joined_rows, key_rows, value_rows, lengths_here):
    row_count = joined_rows.shape[0]
    groups = HEADS // KV_HEADS
    query_width = HEADS * HDIM
    kv_width = KV_HEADS * HDIM
    queries = joined_rows[:, :query_width].reshape(row_count, KV_HEADS, groups, HDIM)
    new_keys = joined_rows[:, query_width : query_width + kv_width].reshape(
        row_count, KV_HEADS, HDIM
    )
    new_values = joined_rows[:, query_width + kv_width :].reshape(row_count, KV_HEADS, HDIM)
    position = lengths_here.astype(jnp.float32)
    queries = rotate(queries.astype(jnp.float32), position[:, None, None]).astype(jnp.bfloat16)
    new_keys = rotate(new_keys.astype(jnp.float32), position[:, None]).astype(jnp.bfloat16)
    score_scale = 1.0 / math.sqrt(HDIM)
    cache_span = key_rows.shape[1]
    cached_keys = key_rows.reshape(row_count, cache_span, KV_HEADS, HDIM)
    cached_values = value_rows.reshape(row_count, cache_span, KV_HEADS, HDIM)
    own_score = (
        jnp.einsum("ngqd,ngd->ngq", queries, new_keys, preferred_element_type=jnp.float32)
        * score_scale
    )
    scores = (
        jnp.einsum("ngqd,nlgd->ngql", queries, cached_keys, preferred_element_type=jnp.float32)
        * score_scale
    )
    live_mask = (jnp.arange(cache_span, dtype=jnp.int32)[None, :] < lengths_here[:, None])[
        :, None, None, :
    ]
    masked = jnp.where(live_mask, scores, masked_score)
    peak = jnp.maximum(jnp.max(masked, axis=-1), own_score)
    weights = jnp.where(live_mask, jnp.exp(masked - peak[..., None]), 0.0)
    sums = jnp.sum(weights, axis=-1)
    weighted = jnp.einsum(
        "ngql,nlgd->ngqd",
        weights.astype(jnp.bfloat16),
        cached_values,
        preferred_element_type=jnp.float32,
    )
    own_weight = jnp.exp(own_score - peak)
    denominator = sums + own_weight
    own_rounded = own_weight.astype(jnp.bfloat16).astype(jnp.float32)
    weighted = weighted + own_rounded[..., None] * new_values.astype(jnp.float32)[:, :, None, :]
    return (weighted / denominator[..., None]).reshape(row_count, query_width).astype(jnp.bfloat16)


def shards(acts, norm_gain, w_qkv, w_out, key_cache, value_cache, cache_lengths, slot_of):
    tokens = acts[0].astype(jnp.float32)
    squares = lax.psum(jnp.sum(tokens * tokens, axis=1), "wide")
    normed = (
        tokens * lax.rsqrt(squares / D + epsilon)[:, None] * norm_gain[0].astype(jnp.float32)
    ).astype(jnp.bfloat16)
    slot_table = slot_of[0]
    request_total = slot_table.shape[0]
    request_at_slot = (
        jnp.zeros((request_total,), jnp.int32)
        .at[slot_table]
        .set(jnp.arange(request_total, dtype=jnp.int32))
    )
    projection = w_qkv[0]
    whole = lax.all_gather(normed, "wide", axis=1, tiled=True)
    columns = jnp.dot(whole, projection, preferred_element_type=jnp.float32).astype(jnp.bfloat16)
    joined_rows = lax.all_to_all(
        columns[request_at_slot], "wide", split_axis=0, concat_axis=1, tiled=True
    )
    attended = attend(joined_rows, key_cache[0], value_cache[0], cache_lengths[0])
    out_weight = w_out[0]
    projected = jnp.dot(
        lax.all_gather(attended, "wide", axis=0, tiled=True),
        out_weight,
        preferred_element_type=jnp.float32,
    )
    updated = (tokens + projected[slot_table]).astype(jnp.bfloat16)
    return passed_along(updated[None], "section", 1)


def solution(mesh):
    placed = (
        P("section", "rep", "wide"),
        P("section", "wide"),
        P("section", None, "wide"),
        P("section", None, "wide"),
        P("section", ("rep", "wide"), None, None),
        P("section", ("rep", "wide"), None, None),
        P("section", ("rep", "wide")),
        P("section", "rep"),
    )
    n, sections = mesh.shape["wide"], mesh.shape["section"]

    def body(*blocks):
        acts, w_qkv, w_out = blocks[0], blocks[2], blocks[3]
        aligned = acts.shape[2] % 1024 == 0 and w_qkv.shape[2] % HDIM == 0
        if n % 2 == 0 and aligned and blocks[4].shape[1] * n == acts.shape[1]:
            return fused(n, sections, *blocks)
        return shards(*blocks)

    return jax.shard_map(
        body, mesh=mesh, in_specs=placed, out_specs=P("section", "rep", "wide"), check_vma=False
    )
```

```python
import functools
import math

import jax
import jax.numpy as jnp
from jax import lax
from jax.experimental import pallas as pl
from jax.experimental.pallas import tpu as pltpu
from jax.sharding import PartitionSpec as P

D = 8192
HEADS = 32
KV_HEADS = 4
HDIM = 128

epsilon = 1e-05
rope_base = 500000.0
masked_score = -1e30

MESH = pl.DeviceIdType.MESH


def tick(
    n, Y, C, sections,
    acts_ref, gain_ref, slot_ref, len_ref, wq_hbm, wo_hbm, k_hbm, v_hbm, out_hbm,
    wq, wo, kc, vc, xa, acc, js, jr, sqs, sqr, qs, at, ga, res, bias, fin,
    wq_sem, wo_sem, k_sem, v_sem,
    x_sz, x_sy, x_rv, j_sn, j_rv, q_sn, q_rv, a_sz, a_sy, a_rv, o_sn, o_rv,
):
    me = lax.axis_index("wide")
    sec = lax.axis_index("section")
    Z = n // Y
    z, y = me // Y, lax.rem(me, Y)
    other = z * Y + (1 - y)
    rows, width = acts_ref.shape[1], acts_ref.shape[2]
    CK = width // C
    G = KV_HEADS
    heads = HEADS // G
    own = rows // n
    cols = wq.shape[1]
    slabs = cols // HDIM
    out_chunks = res.shape[0]
    OC = res.shape[2]

    barrier = pltpu.get_barrier_semaphore()
    for step in range(1, n):
        pl.semaphore_signal(
            barrier, inc=1, device_id={"wide": lax.rem(me + step, n)}, device_id_type=MESH
        )
    pl.semaphore_signal(
        barrier, inc=1, device_id={"section": lax.rem(sec + 1, sections)}, device_id_type=MESH
    )

    def wq_copy(b):
        at_rows = pl.ds(pl.multiple_of(b * width, width), width)
        return pltpu.make_async_copy(wq_hbm.at[0, at_rows, :], wq.at[at_rows, :], wq_sem.at[b])

    for step in range(n):
        wq_copy(lax.rem(me + step, n)).start()
    k_copy = pltpu.make_async_copy(k_hbm.at[0], kc, k_sem)
    v_copy = pltpu.make_async_copy(v_hbm.at[0], vc, v_sem)
    wo_copy = pltpu.make_async_copy(wo_hbm.at[0], wo, wo_sem)
    k_copy.start()
    v_copy.start()
    wo_copy.start()

    tokens = acts_ref[0].astype(jnp.float32)
    gained = (tokens * gain_ref[...].astype(jnp.float32)).astype(jnp.bfloat16)
    for c in range(C):
        xa[me, c] = gained[:, c * CK : (c + 1) * CK]
    squares = jnp.sum(tokens * tokens, axis=1, keepdims=True)
    sub = lax.broadcasted_iota(jnp.int32, (rows, rows), 0)
    lane = lax.broadcasted_iota(jnp.int32, (rows, rows), 1)
    square_row = jnp.sum(jnp.where(sub == lane, squares, 0.0), axis=0, keepdims=True)
    to_slot_mask = sub == slot_ref[...]
    square_slot = jnp.sum(jnp.where(to_slot_mask, square_row, 0.0), axis=1, keepdims=True)
    square_wide = jnp.broadcast_to(square_slot, (rows, HDIM))
    for o in range(n):
        sqs[o] = square_wide[o * own : (o + 1) * own]
    to_slot_f = jnp.where(to_slot_mask, 1.0, 0.0)
    to_slot = to_slot_f.astype(jnp.bfloat16)
    to_request = to_slot_f.T.astype(jnp.bfloat16)

    pl.semaphore_wait(barrier, n)

    def remote(src, dst, send, recv, target):
        return pltpu.make_async_remote_copy(
            src_ref=src, dst_ref=dst, send_sem=send, recv_sem=recv,
            device_id={"wide": target}, device_id_type=MESH,
        )

    def x_z(dz, c, way):
        b = (z - way * dz) * Y + y
        return remote(
            xa.at[b, c], xa.at[b, c], x_sz.at[dz * 2 + (way + 1) // 2, c], x_rv.at[b, c],
            (z + way) * Y + y,
        )

    def x_on(dz, way):
        source, onward = z - way * dz, z + way
        return (source >= 0) & (source < Z) & (onward >= 0) & (onward < Z)

    def x_pass(dz, c, way):
        @pl.when(x_on(dz, way))
        def _():
            x_z(dz, c, way).start()

    def x_sent(dz, c, way):
        @pl.when(x_on(dz, way))
        def _():
            x_z(dz, c, way).wait_send()

    def x_y(zb, c):
        b = zb * Y + y
        return remote(xa.at[b, c], xa.at[b, c], x_sy.at[zb, c], x_rv.at[b, c], other)

    def x_wait(b, c):
        remote(xa.at[b, c], xa.at[b, c], x_sy.at[0, c], x_rv.at[b, c], other).wait_recv()

    for c in range(C):
        x_pass(0, c, 1)
        x_pass(0, c, -1)
        x_y(z, c).start()

    def q_copy(step):
        o = lax.rem(me + step, n)
        return remote(sqs.at[o], sqr.at[me], q_sn.at[step], q_rv.at[me], o)

    for step in range(1, n):
        q_copy(step).start()
    sqr[me] = sqs[me]

    def piece(b, c):
        at_rows = pl.ds(pl.multiple_of(b * width + c * CK, CK), CK)
        return jnp.dot(xa[b, c], wq[at_rows, :], preferred_element_type=jnp.float32)

    for step in range(n):
        wq_copy(lax.rem(me + step, n)).wait()

    total = piece(me, 0)
    for c in range(1, C):
        total += piece(me, c)
    acc[...] = total

    def gather_step(i, carry):
        d, c = i // C + 1, lax.rem(i, C)
        for way in (1, -1):
            source = z - way * d

            @pl.when((source >= 0) & (source < Z))
            def _():
                x_wait(source * Y + y, c)
                x_pass(d, c, way)
                x_y(source, c).start()

        for way in (1, -1):
            source = z - way * d

            @pl.when((source >= 0) & (source < Z))
            def _():
                acc[...] += piece(source * Y + y, c)

        for way in (1, -1):
            source = z - way * (d - 1)

            @pl.when((source >= 0) & (source < Z) & ((d > 1) | (way == 1)))
            def _():
                x_wait(source * Y + (1 - y), c)
                acc[...] += piece(source * Y + (1 - y), c)

        return carry

    lax.fori_loop(0, Z * C, gather_step, 0)

    by_slot = jnp.dot(to_slot, acc[...].astype(jnp.bfloat16), preferred_element_type=jnp.float32)
    for o in range(n):
        js[o] = by_slot[o * own : (o + 1) * own].astype(jnp.bfloat16)

    def j_copy(step):
        o = lax.rem(me + step, n)
        return remote(js.at[o], jr.at[me], j_sn.at[step], j_rv.at[me], o)

    for step in range(1, n):
        j_copy(step).start()
    jr[me] = js[me]

    row_of = lax.broadcasted_iota(jnp.int32, (own, HDIM), 0)
    lane_of = lax.broadcasted_iota(jnp.int32, (own, HDIM), 1)
    position = jnp.zeros((own, HDIM), jnp.int32)
    for r in range(own):
        position = jnp.where(row_of == r, len_ref[0, r], position)
    half = lax.rem(lane_of, HDIM // 2).astype(jnp.float32) * (2.0 / HDIM)
    angle = position.astype(jnp.float32) * jnp.exp(-math.log(rope_base) * half)
    cosine = jnp.cos(angle)
    sine = jnp.where(lane_of < HDIM // 2, -jnp.sin(angle), jnp.sin(angle))
    place = lax.broadcasted_iota(jnp.int32, (heads, kc.shape[1]), 1)
    for r in range(own):
        bias[r * heads : (r + 1) * heads] = jnp.where(place < len_ref[0, r], 0.0, masked_score)
    fin[...] = acts_ref[0].astype(jnp.float32)
    k_copy.wait()
    v_copy.wait()
    wo_copy.wait()

    for step in range(1, n):
        b = lax.rem(me + step, n)
        remote(sqs.at[b], sqr.at[b], q_sn.at[step], q_rv.at[b], b).wait_recv()
    square_sum = sqr[0]
    for b in range(1, n):
        square_sum += sqr[b]
    scale = lax.rsqrt(square_sum / D + epsilon)
    for step in range(1, n):
        b = lax.rem(me + step, n)
        remote(js.at[b], jr.at[b], j_sn.at[step], j_rv.at[b], b).wait_recv()
    for b in range(n):
        for k in range(slabs):
            feature = b * slabs + k
            slab = jr[b, :, k * HDIM : (k + 1) * HDIM].astype(jnp.float32) * scale
            if feature < HEADS + G:
                turned = slab * cosine + pltpu.roll(slab, HDIM // 2, 1) * sine
                slab = turned.astype(jnp.bfloat16).astype(jnp.float32)
            else:
                slab = slab.astype(jnp.bfloat16).astype(jnp.float32)
            qs[:, feature, :] = slab

    def a_z(g, dz):
        return remote(
            ga.at[g, me], ga.at[g, me], a_sz.at[g, dz], a_rv.at[g, me],
            lax.rem(z + dz, Z) * Y + y,
        )

    def a_y(g, zb):
        b = zb * Y + y
        return remote(ga.at[g, b], ga.at[g, b], a_sy.at[g, zb], a_rv.at[g, b], other)

    def a_wait(g, b):
        remote(ga.at[g, b], ga.at[g, b], a_sy.at[g, 0], a_rv.at[g, b], other).wait_recv()

    def relay(g):
        for dz in range(1, Z):
            zb = lax.rem(z + dz, Z)
            a_wait(g, zb * Y + y)
            a_y(g, zb).start()

    def o_copy(c):
        return pltpu.make_async_remote_copy(
            src_ref=res.at[c],
            dst_ref=out_hbm.at[0, :, pl.ds(c * OC, OC)],
            send_sem=o_sn.at[c],
            recv_sem=o_rv.at[c],
            device_id={"section": lax.rem(sec + 1, sections)},
            device_id_type=MESH,
        )

    score_scale = 1.0 / math.sqrt(HDIM)
    depth = heads * HDIM
    stacked = own * heads

    def queries_of(g):
        return qs[:, g * heads : (g + 1) * heads, :].reshape(stacked, HDIM)

    def spread(slab):
        return jnp.broadcast_to(qs[:, slab : slab + 1, :], (own, heads, HDIM)).reshape(
            stacked, HDIM
        )

    def scores_of(g):
        lanes = slice(g * HDIM, (g + 1) * HDIM)
        return jnp.concatenate(
            [
                lax.dot_general(
                    qs[r, g * heads : (g + 1) * heads, :].astype(jnp.bfloat16), kc[r, :, lanes],
                    (((1,), (1,)), ((), ())), preferred_element_type=jnp.float32,
                )
                for r in range(own)
            ],
            axis=0,
        )

    def mixed_of(g):
        for dz in range(Z):
            a_wait(g, lax.rem(z + dz, Z) * Y + (1 - y))
        block = ga[g].astype(jnp.float32).reshape(rows, depth).astype(jnp.bfloat16)
        return jnp.dot(to_request, block, preferred_element_type=jnp.float32).astype(jnp.bfloat16)

    def project(g):
        mixed = mixed_of(g)
        for c in range(out_chunks):
            at_cols = slice(c * OC, (c + 1) * OC)
            fin[:, at_cols] += jnp.dot(
                mixed, wo[g * depth : (g + 1) * depth, at_cols], preferred_element_type=jnp.float32
            )

    upcoming = scores_of(0)
    for g in range(G):
        scores = upcoming
        if g < G - 1:
            upcoming = scores_of(g + 1)
        lanes = slice(g * HDIM, (g + 1) * HDIM)
        own_score = (
            jnp.sum(queries_of(g) * spread(HEADS + g), axis=1, keepdims=True) * score_scale
        )
        masked = scores * score_scale + bias[...]
        peak = jnp.maximum(jnp.max(masked, axis=1, keepdims=True), own_score)
        weights = jnp.exp(masked - peak)
        own_weight = jnp.exp(own_score - peak)
        denominator = jnp.sum(weights, axis=1, keepdims=True) + own_weight
        weighted = jnp.concatenate(
            [
                jnp.dot(
                    weights[r * heads : (r + 1) * heads].astype(jnp.bfloat16), vc[r, :, lanes],
                    preferred_element_type=jnp.float32,
                )
                for r in range(own)
            ],
            axis=0,
        )
        weighted += own_weight.astype(jnp.bfloat16).astype(jnp.float32) * spread(HEADS + G + g)
        at[g] = (weighted / denominator).reshape(own, heads, HDIM)
        for h in range(heads):
            ga[g, me, :, h * HDIM : (h + 1) * HDIM] = at[g, :, h, :].astype(jnp.bfloat16)
        a_y(g, z).start()
        for dz in range(1, Z):
            a_z(g, dz).start()
        if g >= 2:
            relay(g - 2)
    for g in range(max(G - 2, 0), G):
        relay(g)
        if g < G - 1:
            project(g - (G - 2))
    for g in range(1, G - 1):
        project(g)
    mixed = mixed_of(G - 1)
    for c in range(out_chunks):
        at_cols = slice(c * OC, (c + 1) * OC)
        part = fin[:, at_cols] + jnp.dot(
            mixed, wo[(G - 1) * depth :, at_cols], preferred_element_type=jnp.float32
        )
        res[c] = part.astype(jnp.bfloat16)
        o_copy(c).start()

    for c in range(C):
        for dz in range(Z - 1):
            x_sent(dz, c, 1)
            x_sent(dz, c, -1)
        for zb in range(Z):
            x_y(zb, c).wait_send()
    for step in range(1, n):
        q_copy(step).wait_send()
        j_copy(step).wait_send()
    for g in range(G):
        for dz in range(1, Z):
            a_z(g, dz).wait_send()
        for zb in range(Z):
            a_y(g, zb).wait_send()
    for c in range(out_chunks):
        o_copy(c).wait()


def fused(n, sections, acts, norm_gain, w_qkv, w_out, key_cache, value_cache, cache_lengths, slot_of):
    Y, C, out_chunks = 2, 2, 4
    rows, width = acts.shape[1:]
    own, span, kv_width = key_cache.shape[1:]
    cols = w_qkv.shape[2]
    G = KV_HEADS
    heads = HEADS // G
    Z = n // Y
    vmem = pl.BlockSpec(memory_space=pltpu.VMEM)
    smem = pl.BlockSpec(memory_space=pltpu.SMEM)
    anywhere = pl.BlockSpec(memory_space=pl.ANY)
    bf16, f32 = jnp.bfloat16, jnp.float32
    dma = pltpu.SemaphoreType.DMA
    return pl.pallas_call(
        functools.partial(tick, n, Y, C, sections),
        out_shape=jax.ShapeDtypeStruct(acts.shape, bf16),
        in_specs=[vmem, vmem, vmem, smem, anywhere, anywhere, anywhere, anywhere],
        out_specs=anywhere,
        scratch_shapes=[
            pltpu.VMEM(w_qkv.shape[1:], bf16),
            pltpu.VMEM(w_out.shape[1:], bf16),
            pltpu.VMEM(key_cache.shape[1:], bf16),
            pltpu.VMEM(value_cache.shape[1:], bf16),
            pltpu.VMEM((n, C, rows, width // C), bf16),
            pltpu.VMEM((rows, cols), f32),
            pltpu.VMEM((n, own, cols), bf16),
            pltpu.VMEM((n, own, cols), bf16),
            pltpu.VMEM((n, own, HDIM), f32),
            pltpu.VMEM((n, own, HDIM), f32),
            pltpu.VMEM((own, HEADS + 2 * G, HDIM), f32),
            pltpu.VMEM((G, own, heads, HDIM), f32),
            pltpu.VMEM((G, n, own, heads * HDIM), bf16),
            pltpu.VMEM((out_chunks, rows, width // out_chunks), bf16),
            pltpu.VMEM((own * heads, span), f32),
            pltpu.VMEM((rows, width), f32),
            dma((n,)), dma, dma, dma,
            dma((2 * Z, C)), dma((Z, C)), dma((n, C)),
            dma((n,)), dma((n,)), dma((n,)), dma((n,)),
            dma((G, Z)), dma((G, Z)), dma((G, n)),
            dma((out_chunks,)), dma((out_chunks,)),
        ],
        compiler_params=pltpu.CompilerParams(
            collective_id=0, has_side_effects=True, vmem_limit_bytes=60 * 1024 * 1024
        ),
    )(acts, norm_gain, slot_of, cache_lengths, w_qkv, w_out, key_cache, value_cache)


def passed_along(value, axis, steps):
    count = lax.axis_size(axis)
    pairs = [(source, (source + steps) % count) for source in range(count)]
    return lax.ppermute(value, axis, pairs)


def rotate(values, position):
    half_dim = HDIM // 2
    exponent = jnp.arange(half_dim, dtype=jnp.float32) * (2.0 / HDIM)
    frequency = jnp.exp(-math.log(rope_base) * exponent)
    angle = position[..., None] * frequency
    cosine = jnp.cos(angle)
    sine = jnp.sin(angle)
    first_half = values[..., :half_dim]
    second_half = values[..., half_dim:]
    return jnp.concatenate(
        [first_half * cosine - second_half * sine, second_half * cosine + first_half * sine],
        axis=-1,
    )


def attend(joined_rows, key_rows, value_rows, lengths_here):
    row_count = joined_rows.shape[0]
    groups = HEADS // KV_HEADS
    query_width = HEADS * HDIM
    kv_width = KV_HEADS * HDIM
    queries = joined_rows[:, :query_width].reshape(row_count, KV_HEADS, groups, HDIM)
    new_keys = joined_rows[:, query_width : query_width + kv_width].reshape(
        row_count, KV_HEADS, HDIM
    )
    new_values = joined_rows[:, query_width + kv_width :].reshape(row_count, KV_HEADS, HDIM)
    position = lengths_here.astype(jnp.float32)
    queries = rotate(queries.astype(jnp.float32), position[:, None, None]).astype(jnp.bfloat16)
    new_keys = rotate(new_keys.astype(jnp.float32), position[:, None]).astype(jnp.bfloat16)
    score_scale = 1.0 / math.sqrt(HDIM)
    cache_span = key_rows.shape[1]
    cached_keys = key_rows.reshape(row_count, cache_span, KV_HEADS, HDIM)
    cached_values = value_rows.reshape(row_count, cache_span, KV_HEADS, HDIM)
    own_score = (
        jnp.einsum("ngqd,ngd->ngq", queries, new_keys, preferred_element_type=jnp.float32)
        * score_scale
    )
    scores = (
        jnp.einsum("ngqd,nlgd->ngql", queries, cached_keys, preferred_element_type=jnp.float32)
        * score_scale
    )
    live_mask = (jnp.arange(cache_span, dtype=jnp.int32)[None, :] < lengths_here[:, None])[
        :, None, None, :
    ]
    masked = jnp.where(live_mask, scores, masked_score)
    peak = jnp.maximum(jnp.max(masked, axis=-1), own_score)
    weights = jnp.where(live_mask, jnp.exp(masked - peak[..., None]), 0.0)
    sums = jnp.sum(weights, axis=-1)
    weighted = jnp.einsum(
        "ngql,nlgd->ngqd",
        weights.astype(jnp.bfloat16),
        cached_values,
        preferred_element_type=jnp.float32,
    )
    own_weight = jnp.exp(own_score - peak)
    denominator = sums + own_weight
    own_rounded = own_weight.astype(jnp.bfloat16).astype(jnp.float32)
    weighted = weighted + own_rounded[..., None] * new_values.astype(jnp.float32)[:, :, None, :]
    return (weighted / denominator[..., None]).reshape(row_count, query_width).astype(jnp.bfloat16)


def shards(acts, norm_gain, w_qkv, w_out, key_cache, value_cache, cache_lengths, slot_of):
    tokens = acts[0].astype(jnp.float32)
    squares = lax.psum(jnp.sum(tokens * tokens, axis=1), "wide")
    normed = (
        tokens * lax.rsqrt(squares / D + epsilon)[:, None] * norm_gain[0].astype(jnp.float32)
    ).astype(jnp.bfloat16)
    slot_table = slot_of[0]
    request_total = slot_table.shape[0]
    request_at_slot = (
        jnp.zeros((request_total,), jnp.int32)
        .at[slot_table]
        .set(jnp.arange(request_total, dtype=jnp.int32))
    )
    projection = w_qkv[0]
    whole = lax.all_gather(normed, "wide", axis=1, tiled=True)
    columns = jnp.dot(whole, projection, preferred_element_type=jnp.float32).astype(jnp.bfloat16)
    joined_rows = lax.all_to_all(
        columns[request_at_slot], "wide", split_axis=0, concat_axis=1, tiled=True
    )
    attended = attend(joined_rows, key_cache[0], value_cache[0], cache_lengths[0])
    out_weight = w_out[0]
    projected = jnp.dot(
        lax.all_gather(attended, "wide", axis=0, tiled=True),
        out_weight,
        preferred_element_type=jnp.float32,
    )
    updated = (tokens + projected[slot_table]).astype(jnp.bfloat16)
    return passed_along(updated[None], "section", 1)


def solution(mesh):
    placed = (
        P("section", "rep", "wide"),
        P("section", "wide"),
        P("section", None, "wide"),
        P("section", None, "wide"),
        P("section", ("rep", "wide"), None, None),
        P("section", ("rep", "wide"), None, None),
        P("section", ("rep", "wide")),
        P("section", "rep"),
    )
    n, sections = mesh.shape["wide"], mesh.shape["section"]

    def body(*blocks):
        acts, w_qkv, w_out = blocks[0], blocks[2], blocks[3]
        aligned = acts.shape[2] % 1024 == 0 and w_qkv.shape[2] % HDIM == 0
        if n % 2 == 0 and aligned and blocks[4].shape[1] * n == acts.shape[1]:
            return fused(n, sections, *blocks)
        return shards(*blocks)

    return jax.shard_map(
        body, mesh=mesh, in_specs=placed, out_specs=P("section", "rep", "wide"), check_vma=False
    )
```
